32 devices in a mesh: rep: 2 (over z, core), dp: 16 (over x, y).
Axes of the slice: x: 4, y: 4, z: 1, core: 2. Of those that a mesh axis runs over, the one named last changes fastest.
The devices are a block of a 4x4x8 slice.
Arguments:
- x: bfloat16 [32, 2048, 768], P(('rep', 'dp')), parts along dimension 0
- dy: bfloat16 [32, 2048, 768], P(('rep', 'dp')), parts along dimension 0
- wq: bfloat16 [2, 768, 768], P(None, 'dp')
- wk: bfloat16 [2, 768, 256], P(None, 'dp')
- wv: bfloat16 [2, 768, 256], P(None, 'dp')
- wo: bfloat16 [2, 768, 768], P(None, 'dp')
- w_gate: bfloat16 [2, 768, 2048], P(None, 'dp')
- w_up: bfloat16 [2, 768, 2048], P(None, 'dp')
- w_down: bfloat16 [2, 2048, 768], P(None, 'dp')
- m_wq: float32 [2, 768, 768], P(None, 'dp')
- m_wk: float32 [2, 768, 256], P(None, 'dp')
- m_wv: float32 [2, 768, 256], P(None, 'dp')
- m_wo: float32 [2, 768, 768], P(None, 'dp')
- m_w_gate: float32 [2, 768, 2048], P(None, 'dp')
- m_w_up: float32 [2, 768, 2048], P(None, 'dp')
- m_w_down: float32 [2, 2048, 768], P(None, 'dp')
- v_wq: float32 [2, 768, 768], P(None, 'dp')
- v_wk: float32 [2, 768, 256], P(None, 'dp')
- v_wv: float32 [2, 768, 256], P(None, 'dp')
- v_wo: float32 [2, 768, 768], P(None, 'dp')
- v_w_gate: float32 [2, 768, 2048], P(None, 'dp')
- v_w_up: float32 [2, 768, 2048], P(None, 'dp')
- v_w_down: float32 [2, 2048, 768], P(None, 'dp')
Outputs:
- output 1: bfloat16 [4, 768, 768], P('rep', 'dp'), parts along dimension 0
- output 2: bfloat16 [4, 768, 256], P('rep', 'dp'), parts along dimension 0
- output 3: bfloat16 [4, 768, 256], P('rep', 'dp'), parts along dimension 0
- output 4: bfloat16 [4, 768, 768], P('rep', 'dp'), parts along dimension 0
- output 5: bfloat16 [4, 768, 2048], P('rep', 'dp'), parts along dimension 0
- output 6: bfloat16 [4, 768, 2048], P('rep', 'dp'), parts along dimension 0
- output 7: bfloat16 [4, 2048, 768], P('rep', 'dp'), parts along dimension 0
- output 8: float32 [4, 768, 768], P('rep', 'dp'), parts along dimension 0
- output 9: float32 [4, 768, 256], P('rep', 'dp'), parts along dimension 0
- output 10: float32 [4, 768, 256], P('rep', 'dp'), parts along dimension 0
- output 11: float32 [4, 768, 768], P('rep', 'dp'), parts along dimension 0
- output 12: float32 [4, 768, 2048], P('rep', 'dp'), parts along dimension 0
- output 13: float32 [4, 768, 2048], P('rep', 'dp'), parts along dimension 0
- output 14: float32 [4, 2048, 768], P('rep', 'dp'), parts along dimension 0
- output 15: float32 [4, 768, 768], P('rep', 'dp'), parts along dimension 0
- output 16: float32 [4, 768, 256], P('rep', 'dp'), parts along dimension 0
- output 17: float32 [4, 768, 256], P('rep', 'dp'), parts along dimension 0
- output 18: float32 [4, 768, 768], P('rep', 'dp'), parts along dimension 0
- output 19: float32 [4, 768, 2048], P('rep', 'dp'), parts along dimension 0
- output 20: float32 [4, 768, 2048], P('rep', 'dp'), parts along dimension 0
- output 21: float32 [4, 2048, 768], P('rep', 'dp'), parts along dimension 0
There are 2 independent parts. The reference program is written for one: setup_inputs(seed, part) draws one part's arguments, and reference() takes and returns one part's arrays. A program takes and returns all parts, laid end to end along the dimension named above; an argument that names none is the same for every part.
All inputs are finite; a program needn't handle non-finite values.
Results may differ from the reference program's by a relative error of at most 0.0249.
Values are sent between devices in bfloat16 or wider.
A program may use at most 768 MiB of HBM per device.

```python
import jax
import jax.numpy as jnp
from jax import lax

SEQUENCES = 16
TOKENS = 2048
D = 768
HEADS = 6
KV_HEADS = 2
HEAD = 128
FF = 2048
LAYERS = 2
THETA = 10000
NAMES = ("wq", "wk", "wv", "wo", "w_gate", "w_up", "w_down")
SHAPES = {
    "wq": (LAYERS, D, HEADS * HEAD),
    "wk": (LAYERS, D, KV_HEADS * HEAD),
    "wv": (LAYERS, D, KV_HEADS * HEAD),
    "wo": (LAYERS, HEADS * HEAD, D),
    "w_gate": (LAYERS, D, FF),
    "w_up": (LAYERS, D, FF),
    "w_down": (LAYERS, FF, D),
}


def bump(key, n, height):
    away = (jnp.arange(n, dtype=jnp.int32) - jax.random.randint(key, (), 0, n, jnp.int32)) % n
    return jnp.where(away < n // 8, height, 1.0)


def together(key, own, strength):
    shared = jax.random.normal(key, own.shape[1:], jnp.float32)
    return (own + strength * shared) * lax.rsqrt(1 + strength * strength)


def setup_inputs(seed: int = 0, part: int = 0) -> dict:
    kx, kdy, ka, kb, kz, kf, kh, kl, *keys = jax.random.split(jax.random.key(seed), 8 + 3 * len(NAMES))
    kx, kdy, ka, kb = (jax.random.fold_in(k, part) for k in (kx, kdy, ka, kb))
    kw, km, kv = (keys[i::3] for i in range(3))
    shape = (SEQUENCES, TOKENS, D)
    much_x, much_dy = jax.random.uniform(kz, (2,), jnp.float32, 0.0, 1.0)
    loud = 2.0 ** jax.random.uniform(jax.random.fold_in(kz, 1), (), jnp.float32, -1.0, 2.0)
    layers = 2.0 ** jax.random.uniform(kl, (LAYERS, 1, 1), jnp.float32, -1.0, 1.0)
    times = {"wq": 1.0, "wk": 1.0, "wv": 2.0, "wo": layers, "w_gate": 1.0, "w_up": bump(kh, FF, 4.0), "w_down": layers}
    x = together(ka, jax.random.normal(kx, shape, jnp.float32), much_x) * bump(kf, D, 4.0)
    dy = together(kb, jax.random.normal(kdy, shape, jnp.float32), much_dy)
    drawn = {"x": x.astype(jnp.bfloat16), "dy": (loud * dy * (SEQUENCES * TOKENS) ** -0.5).astype(jnp.bfloat16)}
    for key, name in zip(kw, NAMES, strict=True):
        drawn[name] = (jax.random.normal(key, SHAPES[name], jnp.float32) * SHAPES[name][1] ** -0.5 * times[name]).astype(jnp.bfloat16)
    for key, name in zip(km, NAMES, strict=True):
        drawn[f"m_{name}"] = 0.1 * jax.random.normal(key, SHAPES[name], jnp.float32)
    for key, name in zip(kv, NAMES, strict=True):
        drawn[f"v_{name}"] = jax.random.uniform(key, SHAPES[name], jnp.float32, 0.02, 0.06)
    return drawn


def matmul(a, w):
    return jnp.dot(a, w, preferred_element_type=jnp.float32).astype(jnp.bfloat16)


def normed(h):
    wide = h.astype(jnp.float32)
    scale = lax.rsqrt(jnp.mean(wide**2, -1, keepdims=True) + 1e-6)
    return (wide * scale).astype(jnp.bfloat16)


def turned(t, theta):
    half = t.shape[-1] // 2
    angle = jnp.arange(t.shape[0], dtype=jnp.float32)[:, None] * theta ** (-jnp.arange(half, dtype=jnp.float32) / half)
    cos, sin = jnp.cos(angle)[:, None], jnp.sin(angle)[:, None]
    a, b = t[..., :half].astype(jnp.float32), t[..., half:].astype(jnp.float32)
    return jnp.concatenate([a * cos - b * sin, b * cos + a * sin], -1).astype(jnp.bfloat16)


def seen_by(q, k, v):
    tokens, kv = q.shape[0], k.shape[1]
    q = q.reshape(tokens, kv, -1, q.shape[-1])
    scores = jnp.einsum("tgsd,ugd->gstu", q.astype(jnp.float32), k.astype(jnp.float32)) * q.shape[-1] ** -0.5
    place = jnp.arange(tokens)
    weights = jax.nn.softmax(jnp.where(place[:, None] >= place, scores, -jnp.inf), -1).astype(jnp.bfloat16)
    return jnp.einsum("gstu,ugd->tgsd", weights.astype(jnp.float32), v.astype(jnp.float32)).astype(jnp.bfloat16).reshape(tokens, -1)


def layer(h, w):
    a = normed(h)
    q, k = (turned(matmul(a, w[name]).reshape(h.shape[0], -1, HEAD), THETA) for name in ("wq", "wk"))
    h = h + matmul(seen_by(q, k, matmul(a, w["wv"]).reshape(h.shape[0], -1, HEAD)), w["wo"])
    b = normed(h)
    gate = jnp.dot(b, w["w_gate"], preferred_element_type=jnp.float32)
    up = jnp.dot(b, w["w_up"], preferred_element_type=jnp.float32)
    return h + matmul((jax.nn.silu(gate) * up).astype(jnp.bfloat16), w["w_down"])


def adamw(w, m, v, g):
    m = 0.9 * m + 0.1 * g
    v = 0.95 * v + 0.05 * g * g
    step = m * lax.rsqrt(v + 1e-8) + 0.1 * w
    return (w - 0.02 * step).astype(jnp.bfloat16), m, v


def clipped(gradients, sum_of_squares, count):
    factor = jnp.minimum(1.0, 0.5 * lax.rsqrt(sum_of_squares / count + 1e-30))
    return [g * factor for g in gradients]


def stack(weights, h):
    return lax.scan(lambda h, w: (layer(h, w), None), h, weights)[0]


def reference(x, dy, wq, wk, wv, wo, w_gate, w_up, w_down, m_wq, m_wk, m_wv, m_wo, m_w_gate, m_w_up, m_w_down, v_wq, v_wk, v_wv, v_wo, v_w_gate, v_w_up, v_w_down):
    weights = dict(zip(NAMES, (wq, wk, wv, wo, w_gate, w_up, w_down), strict=True))

    def take(so_far, sequence):
        h, by_y = sequence
        _, back = jax.vjp(stack, weights, h)
        by_weights, by_h = back(by_y)
        return jax.tree.map(lambda total, term: total + term.astype(jnp.float32), so_far, by_weights), by_h

    none_yet = {name: jnp.zeros(w.shape, jnp.float32) for name, w in weights.items()}
    by_weights, by_x = lax.scan(take, none_yet, (x, dy))
    gradients = [by_weights[name].astype(jnp.bfloat16).astype(jnp.float32) for name in NAMES]
    gradients = clipped(gradients, sum(jnp.sum(g * g) for g in gradients), sum(g.size for g in gradients))
    first = (m_wq, m_wk, m_wv, m_wo, m_w_gate, m_w_up, m_w_down)
    second = (v_wq, v_wk, v_wv, v_wo, v_w_gate, v_w_up, v_w_down)
    new = [adamw(weights[name].astype(jnp.float32), m, v, g) for name, m, v, g in zip(NAMES, first, second, gradients, strict=True)]
    return tuple(one[which] for which in range(3) for one in new)
```

```python
import functools
import math

import jax
import jax.numpy as jnp
from jax import lax
from jax.experimental import pallas as pl
from jax.experimental.pallas import tpu as pltpu

NEG = -1e30
HIDDEN = 2 * NEG
LOG2E = 1.4426950408889634
VMEM = 56 * 2**20
STRIP = 512


def _fit(size, want, unit=128):
    return max(n for n in range(unit, max(min(want, size), unit) + 1, unit) if size % n == 0)


def _dot(a, b, ca, cb):
    return lax.dot_general(a, b, (((ca,), (cb,)), ((), ())), preferred_element_type=jnp.float32)


def _gap(bk, cols, bq):
    return lax.rem(lax.broadcasted_iota(jnp.int32, (bk, cols), 1), bq) - lax.broadcasted_iota(jnp.int32, (bk, cols), 0)


def _row(ref, i):
    return jnp.concatenate([ref[i, n : n + 1, :] for n in range(ref.shape[1])], axis=1)


def _blocks(block, iq, bq, bk):
    whole, last = lax.div(iq * bq + 1, bk), lax.div(iq * bq + bq - 1 + bk, bk)
    lax.fori_loop(0, whole, lambda j, _: block(j, False), None)
    lax.fori_loop(whole, last, lambda j, _: block(j, True), None)


def _forward(q_ref, k_ref, v_ref, o_ref, lse_ref, top_s, mix_s, gap_s, *, scale, bk):
    kb, g, bq, d = q_ref.shape
    cols = g * bq
    iq = pl.program_id(0)
    e = scale * LOG2E
    wide = _fit(cols, STRIP)
    pieces = [(i, at) for i in range(kb) for at in range(0, cols, wide)]

    @pl.when(iq == 0)
    def _():
        gap_s[:] = _gap(bk, cols, bq)

    top_s[:] = jnp.full_like(top_s, NEG)
    mix_s[:] = jnp.zeros_like(mix_s)
    ones = jnp.ones((8, bk), jnp.bfloat16)

    def block(j, masked):
        here = pl.ds(j * bk, bk)
        scores = [_dot(k_ref[i, here, :], q_ref[i].reshape(cols, d)[at : at + wide, :], 1, 1) for i, at in pieces]
        ok = gap_s[:] >= j * bk - iq * bq if masked else None
        weights, keeps = [], []
        for (i, at), s in zip(pieces, scores):
            if masked:
                s = jnp.where(ok[:, at : at + wide], s, HIDDEN)
            old = top_s[i : i + 1, at : at + wide]
            top = jnp.maximum(old, s.max(axis=0, keepdims=True))
            top_s[i : i + 1, at : at + wide] = top
            weights.append(jnp.exp2((s - top) * e).astype(jnp.bfloat16))
            keeps.append(jnp.exp2((old - top) * e))
        for (i, at), p, keep in zip(pieces, weights, keeps):
            values = jnp.concatenate([v_ref[i, here, :].T, ones], axis=0)
            mix_s[i, :, at : at + wide] = mix_s[i, :, at : at + wide] * keep + _dot(values, p, 1, 0)

    _blocks(block, iq, bq, bk)
    for i in range(kb):
        total = mix_s[i, d : d + 1, :]
        o_ref[i] = (mix_s[i, :d, :] * (1 / total)).T.reshape(g, bq, d).astype(o_ref.dtype)
        lse = top_s[i : i + 1, :] * scale + jnp.log(total)
        for n in range(g):
            lse_ref[i, n : n + 1, :] = lse[:, n * bq : (n + 1) * bq]


def _cost(h, t, width, arrays):
    return pl.CostEstimate(flops=h * t * t * width, transcendentals=h * t * t // 2, bytes_accessed=sum(a.size * a.dtype.itemsize for a in arrays))


def _split(a, kv):
    return a.reshape(kv, -1, *a.shape[1:])


def attend(q, k, v, bq=512, bk=512):
    (h, t, d), kv = q.shape, k.shape[0]
    g = h // kv
    bq, bk = _fit(t, bq), _fit(t, bk)
    queries = pl.BlockSpec((kv, g, bq, d), lambda i: (0, 0, i, 0))
    stats = pl.BlockSpec((kv, g, bq), lambda i: (0, 0, i))
    keys = pl.BlockSpec((kv, t, d), lambda i: (0, 0, 0))
    out, lse = pl.pallas_call(
        functools.partial(_forward, scale=d**-0.5, bk=bk), grid=(t // bq,), in_specs=[queries, keys, keys], out_specs=[queries, stats],
        scratch_shapes=[pltpu.VMEM((kv, g * bq), jnp.float32), pltpu.VMEM((kv, d + 8, g * bq), jnp.float32), pltpu.VMEM((bk, g * bq), jnp.int32)],
        out_shape=[jax.ShapeDtypeStruct((kv, g, t, d), q.dtype), jax.ShapeDtypeStruct((kv, g, t), jnp.float32)],
        compiler_params=pltpu.CompilerParams(dimension_semantics=("arbitrary",), vmem_limit_bytes=VMEM),
        cost_estimate=_cost(h, t, 2 * d, [q, k, v, q]))(_split(q, kv), k, v)
    return out.reshape(h, t, d), lse


def _backward(q_ref, k_ref, v_ref, do_ref, lse_ref, o_ref, dq_ref, dk_ref, dv_ref, dq_s, dk_s, dv_s, gap_s, *, scale, bk):
    kb, g, bq, d = q_ref.shape
    low = q_ref.dtype
    cols = g * bq
    iq = pl.program_id(0)
    e = scale * LOG2E
    wide = _fit(cols, STRIP)
    pieces = [(i, at) for i in range(kb) for at in range(0, cols, wide)]

    @pl.when(iq == 0)
    def _():
        gap_s[:] = _gap(bk, cols, bq)
        dk_s[:] = jnp.zeros_like(dk_s)
        dv_s[:] = jnp.zeros_like(dv_s)

    dq_s[:] = jnp.zeros_like(dq_s)
    lses = [_row(lse_ref, i) * LOG2E for i in range(kb)]
    deltas = [(do_ref[i].reshape(cols, d).astype(jnp.float32) * o_ref[i].reshape(cols, d).astype(jnp.float32)).T.sum(axis=0, keepdims=True)
              for i in range(kb)]

    def block(j, masked):
        here = pl.ds(j * bk, bk)
        qs = [q_ref[i].reshape(cols, d)[at : at + wide, :] for i, at in pieces]
        dos = [do_ref[i].reshape(cols, d)[at : at + wide, :] for i, at in pieces]
        scores = [_dot(k_ref[i, here, :], x, 1, 1) for (i, _), x in zip(pieces, qs)]
        dps = [_dot(v_ref[i, here, :], x, 1, 1) for (i, _), x in zip(pieces, dos)]
        ok = gap_s[:] >= j * bk - iq * bq if masked else None
        for n, (i, at) in enumerate(pieces):
            p = jnp.exp2(scores[n] * e - lses[i][:, at : at + wide])
            if masked:
                p = jnp.where(ok[:, at : at + wide], p, 0.0)
            ds = (p * (dps[n] - deltas[i][:, at : at + wide])).astype(low)
            dv_s[i, here, :] += _dot(p.astype(low), dos[n], 1, 0)
            dk_s[i, here, :] += _dot(ds, qs[n], 1, 0)
            dq_s[i, :, at : at + wide] += _dot(k_ref[i, here, :].T, ds, 1, 0)

    _blocks(block, iq, bq, bk)
    for i in range(kb):
        dq_ref[i] = (dq_s[i] * scale).T.reshape(g, bq, d).astype(dq_ref.dtype)

    @pl.when(iq == pl.num_programs(0) - 1)
    def _():
        dk_ref[:] = (dk_s[:] * scale).astype(dk_ref.dtype)
        dv_ref[:] = dv_s[:].astype(dv_ref.dtype)


def attend_bwd(q, k, v, d_out, lse, out, bq=256, bk=256):
    (h, t, d), kv = q.shape, k.shape[0]
    g = h // kv
    bq, bk = _fit(t, bq), _fit(t, bk)
    queries = pl.BlockSpec((kv, g, bq, d), lambda i: (0, 0, i, 0))
    stats = pl.BlockSpec((kv, g, bq), lambda i: (0, 0, i))
    keys = pl.BlockSpec((kv, t, d), lambda i: (0, 0, 0))
    dq, dk, dv = pl.pallas_call(
        functools.partial(_backward, scale=d**-0.5, bk=bk), grid=(t // bq,), in_specs=[queries, keys, keys, queries, stats, queries],
        out_specs=[queries, keys, keys],
        scratch_shapes=[pltpu.VMEM((kv, d, g * bq), jnp.float32)] + [pltpu.VMEM((kv, t, d), jnp.float32)] * 2 + [pltpu.VMEM((bk, g * bq), jnp.int32)],
        out_shape=[jax.ShapeDtypeStruct((kv, g, t, d), q.dtype)] + [jax.ShapeDtypeStruct((kv, t, d), q.dtype)] * 2,
        compiler_params=pltpu.CompilerParams(dimension_semantics=("arbitrary",), vmem_limit_bytes=VMEM),
        cost_estimate=_cost(h, t, 5 * d, [q, q, k, k, v, v, d_out]))(_split(q, kv), k, v, _split(d_out, kv), lse, _split(out, kv))
    return dq.reshape(h, t, d), dk, dv


import numpy as np
from jax.sharding import PartitionSpec as P

HEAD = 128
THETA = 10000
NAMES = ("wq", "wk", "wv", "wo", "w_gate", "w_up", "w_down")
WIDE = 256
MESH = pl.DeviceIdType.MESH
BF, F32 = jnp.bfloat16, jnp.float32
ANY = pl.BlockSpec(memory_space=pl.ANY)
WHOLE = pl.BlockSpec(memory_space=pltpu.VMEM)

ORDER = ("w_gate", "w_up", "w_down", "wo", "wq", "wk", "wv")


def params(*semantics, limit=VMEM, **more):
    return pltpu.CompilerParams(dimension_semantics=semantics or None, vmem_limit_bytes=limit, **more)


def cost(flops, arrays, transcendentals=0):
    return pl.CostEstimate(flops=int(flops), bytes_accessed=int(sum(a.size * a.dtype.itemsize for a in arrays)), transcendentals=transcendentals)


def nn(a, b):
    return _dot(a, b, 1, 0)


def nt(a, b):
    return _dot(a, b, 1, 1)


def scale_of(wide):
    return lax.rsqrt(jnp.mean(wide * wide, -1, keepdims=True) + 1e-6)


def norm_back(wide, scale, d):
    return scale * d - wide * (scale * scale * scale * jnp.mean(d * wide, -1, keepdims=True))


def layout(weights):
    at, rows = {}, 0
    for name in ORDER:
        _, r, c = weights[name].shape
        at[name] = (rows, r, c // WIDE)
        rows += r * (c // WIDE)
    return at, rows


def pieces_of(source, first, at, name, target, column, sem):
    start, r, count = at[name]
    k = sum(at[other][2] for other in ORDER[: ORDER.index(name)])
    return [pltpu.make_async_copy(source.at[:, pl.ds(start - first + c * r, r), :], target.at[:, :, pl.ds(column + c * WIDE, WIDE)], sem.at[k + c])
            for c in range(count)]


def piece_sems(at):
    return pltpu.SemaphoreType.DMA((sum(at[name][2] for name in ORDER),))


def packed(weights, at, rows, late):
    layers = weights["wq"].shape[0]

    def kernel(*refs):
        ins, outs = dict(zip(ORDER, refs)), refs[len(ORDER):]
        for number in range(layers):
            for name in ORDER:
                start, r, count = at[name]
                out = outs[2 * number + (start >= late)]
                start -= late if start >= late else 0
                for c in range(count):
                    out[start + c * r : start + (c + 1) * r, :] = ins[name][number, :, c * WIDE : (c + 1) * WIDE]

    out = pl.pallas_call(kernel, in_specs=[WHOLE] * 7, out_specs=[WHOLE] * (2 * layers), compiler_params=params(),
                         out_shape=[jax.ShapeDtypeStruct((late, WIDE), BF), jax.ShapeDtypeStruct((rows - late, WIDE), BF)] * layers)(
        *(weights[name] for name in ORDER))
    return out[::2], out[1::2]


def place(side):
    me = lax.axis_index("dp")
    return lax.div(me, side), lax.rem(me, side)


def greet(peers):
    barrier = pltpu.get_barrier_semaphore()
    for peer in peers:
        pl.semaphore_signal(barrier, inc=1, device_id={"dp": peer}, device_id_type=MESH)
    return lambda: pl.semaphore_wait(barrier, len(peers))


def cross(side, i, j):
    return ([i * side + lax.rem(j + d, side) for d in range(1, side)], [lax.rem(i + d, side) * side + j for d in range(1, side)])


def copy_to(peer, source, target, send_sem, recv_sem):
    copy = pltpu.make_async_remote_copy(src_ref=source, dst_ref=target, send_sem=send_sem, recv_sem=recv_sem,
                                        device_id={"dp": peer}, device_id_type=MESH)
    copy.start()
    return copy


def gathered_now(side, block, number):
    rows = block.shape[0]
    cut = -(-rows // 32) * 16
    top, low = pl.ds(0, cut), pl.ds(cut, rows - cut)

    def kernel(x_ref, o_ref, send_sem, recv_sem):
        i, j = place(side)
        row, column = cross(side, i, j)
        greet(row + column)()
        copies = []
        for d in range(1, side):
            copies.append(copy_to(row[d - 1], x_ref.at[top], o_ref.at[i, j, top], send_sem.at[0, d], recv_sem.at[0, d]))
            copies.append(copy_to(column[d - 1], x_ref.at[low], o_ref.at[i, j, low], send_sem.at[1, d], recv_sem.at[1, d]))
        o_ref[i, j] = x_ref[:]
        for copy in copies:
            copy.wait()
        half = side // 2
        ends = ((column[0], column[-1], lambda k, part: o_ref.at[k, part, top], i), (row[0], row[-1], lambda k, part: o_ref.at[part, k, low], j))
        copies, k = [], 2
        for after, before, at, own in ends:
            mine = at(own, pl.ds(0, side))
            copies.append([copy_to(peer, mine, mine, send_sem.at[k, d], recv_sem.at[k, d]) for d, peer in enumerate((after, before))])
            k += 1
        more = []
        for (after, before, at, own), (up, down) in zip(ends, copies):
            up.wait_recv()
            on = at(lax.rem(own + side - 1, side), pl.ds(0, half))
            more.append(copy_to(after, on, on, send_sem.at[k, 0], recv_sem.at[k, 0]))
            down.wait_recv()
            on = at(lax.rem(own + 1, side), pl.ds(half, half))
            more.append(copy_to(before, on, on, send_sem.at[k, 1], recv_sem.at[k, 1]))
            k += 1
        for pair in copies:
            for copy in pair:
                copy.wait_send()
        for copy in more:
            copy.wait()

    out = pl.pallas_call(kernel, in_specs=[WHOLE], out_specs=WHOLE, out_shape=jax.ShapeDtypeStruct((side, side, rows, WIDE), block.dtype),
                         scratch_shapes=[pltpu.SemaphoreType.DMA((6, side))] * 2,
                         cost_estimate=pl.CostEstimate(flops=20_000_000_000, bytes_accessed=side * side * block.size * 2, transcendentals=0),
                         compiler_params=params(collective_id=number, has_side_effects=True))(block)
    return out.reshape(side * side, rows, WIDE)


def squares(x):
    wide = x.astype(F32)
    wide = wide * wide
    return sum(wide[:, c : c + 128].reshape(-1, 8, 128).sum(0) for c in range(0, x.shape[1], 128))


def summed_now(side, terms, others, number):
    _, rows, _ = terms.shape
    cut = -(-rows // 32) * 16
    top, low = pl.ds(0, cut), pl.ds(cut, rows - cut)

    def kernel(t_ref, *refs):
        other_refs = refs[: len(others)]
        g_ref, part_ref, got_a, got_b, sum_a, sum_b, out_a, out_b, more_a, more_b, send_sem, recv_sem, own_sem = refs[len(others):]
        i, j = place(side)
        row, column = cross(side, i, j)
        greet(row + column)()
        copies = [pltpu.make_async_copy(t_ref.at[:, j, top], got_a.at[0], own_sem.at[0]),
                  pltpu.make_async_copy(t_ref.at[i, :, low], got_b.at[0], own_sem.at[1])]
        for copy in copies:
            copy.start()
        for d in range(1, side):
            copies.append(copy_to(row[d - 1], t_ref.at[:, lax.rem(j + d, side), top], got_a.at[d], send_sem.at[0, d], recv_sem.at[0, d]))
            copies.append(copy_to(column[d - 1], t_ref.at[lax.rem(i + d, side), :, low], got_b.at[d], send_sem.at[1, d], recv_sem.at[1, d]))
        part = sum(squares(ref[:]) for ref in other_refs)
        for copy in copies:
            copy.wait()
        for got, total, out in ((got_a, sum_a, out_a), (got_b, sum_b, out_b)):
            total[:] = sum(got[d].astype(F32) for d in range(side))
            out[:] = total[:].astype(BF)
        copies = []
        for d in range(1, side):
            copies.append(copy_to(column[d - 1], out_a.at[lax.rem(i + d, side)], more_a.at[d], send_sem.at[2, d], recv_sem.at[2, d]))
            copies.append(copy_to(row[d - 1], out_b.at[lax.rem(j + d, side)], more_b.at[d], send_sem.at[3, d], recv_sem.at[3, d]))
        for copy in copies:
            copy.wait()
        g_ref[:cut] = (sum_a[i] + sum(more_a[d].astype(F32) for d in range(1, side))).astype(BF)
        part_ref[:] = part + squares(g_ref[:cut])
        g_ref[cut:] = (sum_b[j] + sum(more_b[d].astype(F32) for d in range(1, side))).astype(BF)
        part_ref[:] += squares(g_ref[cut:])

    halves = (cut, rows - cut)
    return pl.pallas_call(
        kernel, in_specs=[ANY] + [WHOLE] * len(others), out_specs=[WHOLE, WHOLE],
        out_shape=[jax.ShapeDtypeStruct((rows, WIDE), BF), jax.ShapeDtypeStruct((8, 128), F32)],
        scratch_shapes=[pltpu.VMEM((side, side, r, WIDE), BF) for r in halves] + [pltpu.VMEM((side, r, WIDE), to) for to in (F32, BF, BF) for r in halves]
        + [pltpu.SemaphoreType.DMA((4, side))] * 2 + [pltpu.SemaphoreType.DMA((2,))],
        cost_estimate=pl.CostEstimate(flops=20_000_000_000, bytes_accessed=terms.size * 2, transcendentals=0),
        compiler_params=params(collective_id=number, has_side_effects=True))(terms.reshape(side, side, rows, WIDE), *others)


def squares_now(n, part, block, number):
    def kernel(part_ref, block_ref, total_ref, sums, send_sem, recv_sem):
        me = lax.axis_index("dp")
        peers = [lax.rem(me + d, n) for d in range(1, n)]
        ready = greet(peers)
        sums[me] = part_ref[:] + squares(block_ref[:])
        ready()
        copies = [copy_to(peers[d - 1], sums.at[me], sums.at[me], send_sem.at[d], recv_sem.at[d]) for d in range(1, n)]
        for copy in copies:
            copy.wait()
        total_ref[:] = sum(sums[i] for i in range(n))

    return pl.pallas_call(
        kernel, in_specs=[WHOLE, WHOLE], out_specs=WHOLE, out_shape=jax.ShapeDtypeStruct((8, 128), F32),
        scratch_shapes=[pltpu.VMEM((n, 8, 128), F32), pltpu.SemaphoreType.DMA((n,)), pltpu.SemaphoreType.DMA((n,))],
        cost_estimate=pl.CostEstimate(flops=5_000_000_000, bytes_accessed=0, transcendentals=0),
        compiler_params=params(collective_id=number, has_side_effects=True))(part, block)


def table(tokens):
    half = HEAD // 2
    angle = np.arange(tokens, dtype=np.float32)[:, None] * np.float32(THETA) ** (-np.arange(half, dtype=np.float32) / np.float32(half))
    cos, sin = np.cos(angle), np.sin(angle)
    return np.concatenate([cos, cos], 1).astype(np.float32), np.concatenate([-sin, sin], 1).astype(np.float32)


def project(h, cos, sin, source, first, at, heads, kv):
    t, d = h.shape
    bt = _fit(t, 512)
    n = source.shape[0]
    wide = (heads + 2 * kv) * HEAD

    def kernel(h_ref, c_ref, s_ref, w_ref, a_ref, q_ref, k_ref, v_ref, w_s, sem):
        @pl.when(pl.program_id(0) == 0)
        def _():
            copies, column = [], 0
            for name in ("wq", "wk", "wv"):
                copies += pieces_of(w_ref, first, at, name, w_s, column, sem)
                column += at[name][2] * WIDE
            for copy in copies:
                copy.start()
            for copy in copies:
                copy.wait()

        x = h_ref[:].astype(F32)
        a = (x * scale_of(x)).astype(BF)
        a_ref[:] = a
        out = nn(a, w_s[:].reshape(d, wide)).astype(BF)
        cos_, sin_ = c_ref[:], s_ref[:]
        for i in range(heads + kv):
            y = out[:, i * HEAD : (i + 1) * HEAD].astype(F32)
            y = (y * cos_ + pltpu.roll(y, HEAD // 2, 1) * sin_).astype(BF)
            if i < heads:
                q_ref[i] = y
            else:
                k_ref[i - heads] = y
        for i in range(kv):
            v_ref[i] = out[:, (heads + kv + i) * HEAD : (heads + kv + i + 1) * HEAD]

    row = pl.BlockSpec((bt, d), lambda i: (i, 0))
    tab = pl.BlockSpec((bt, HEAD), lambda i: (i, 0))
    head = lambda c: pl.BlockSpec((c, bt, HEAD), lambda i: (0, i, 0))
    return pl.pallas_call(
        kernel, grid=(t // bt,), in_specs=[row, tab, tab, ANY], out_specs=[row, head(heads), head(kv), head(kv)],
        out_shape=[jax.ShapeDtypeStruct((t, d), BF)] + [jax.ShapeDtypeStruct((c, t, HEAD), BF) for c in (heads, kv, kv)],
        scratch_shapes=[pltpu.VMEM((n, d // n, wide), BF), piece_sems(at)],
        cost_estimate=cost(2 * t * d * wide, [h, h, h, source]), compiler_params=params("arbitrary"))(h, cos, sin, source)


def sum_scratch(inner, columns, n):
    return [pltpu.VMEM((inner, columns), F32), pltpu.VMEM((n, inner // n * (columns // WIDE), WIDE), BF), pltpu.SemaphoreType.DMA]


def add_grad(acc, left, right):
    @pl.when(pl.program_id(0) == 0)
    def _():
        acc[:] = jnp.zeros_like(acc)

    acc[:] += nn(left.T, right)


def put_packed(total, held, out_ref, first, n, sem):
    r, count = total.shape[0] // n, total.shape[1] // WIDE
    for c in range(count):
        held[:, c * r : (c + 1) * r, :] = total[:, c * WIDE : (c + 1) * WIDE].astype(BF).reshape(n, r, WIDE)
    copy = pltpu.make_async_copy(held, out_ref.at[:, pl.ds(first, count * r), :], sem)
    copy.start()
    copy.wait()


def feed(h, o, source, first, at, dy=None, rows=None, tile=512):
    t, d = h.shape
    heads = o.shape[0]
    n = source.shape[0]
    ff = at["w_gate"][2] * WIDE
    bt, step = _fit(t, tile), _fit(ff, 512)
    last = dy is not None

    def kernel(*refs):
        if last:
            h_ref, o_ref, dy_ref, w_ref, b_ref, act_ref, dgu_ref, dh2_ref, do_ref, t_ref, wo_s, wgu_s, wd_s, acc_s, held_s, out_sem, sem = refs
        else:
            h_ref, o_ref, w_ref, h2_ref, gate_ref, up_ref, out_ref, wo_s, wgu_s, wd_s, act_s, sem = refs
        start = pl.program_id(0) == 0
        groups = [pieces_of(w_ref, first, at, "wo", wo_s, 0, sem),
                  pieces_of(w_ref, first, at, "w_gate", wgu_s, 0, sem) + pieces_of(w_ref, first, at, "w_up", wgu_s, ff, sem),
                  pieces_of(w_ref, first, at, "w_down", wd_s, 0, sem)]

        def ready(i):
            @pl.when(start)
            def _():
                for copy in groups[i]:
                    copy.wait()

        @pl.when(start)
        def _():
            for group in groups:
                for copy in group:
                    copy.start()

        def last_put():
            @pl.when(pl.program_id(0) == pl.num_programs(0) - 1)
            def _():
                put_packed(acc_s, held_s, t_ref, at["wo"][0], n, out_sem)

        mixed = jnp.concatenate([o_ref[i] for i in range(heads)], axis=1)
        ready(0)
        h2 = (h_ref[:].astype(F32) + nn(mixed, wo_s[:].reshape(-1, d)).astype(BF).astype(F32)).astype(BF)
        if not last:
            h2_ref[:] = h2
        wide = h2.astype(F32)
        scale = scale_of(wide)
        b = (wide * scale).astype(BF)
        ready(1)
        if last:
            b_ref[:] = b
            ready(2)
            back(dy_ref[:], b, wide, scale, None, None, wgu_s, wd_s, wo_s, act_ref, dgu_ref, dh2_ref, do_ref, heads, ff, step,
                 mixed, acc_s)
            last_put()
            return
        def columns(k, _):
            here, there = pl.ds(pl.multiple_of(k * step, step), step), pl.ds(pl.multiple_of(ff + k * step, step), step)
            gate = nn(b, wgu_s[:, :, here].reshape(d, step))
            up = nn(b, wgu_s[:, :, there].reshape(d, step))
            gate_ref[:, here] = gate
            up_ref[:, here] = up
            act_s[:, here] = (gate * jax.nn.sigmoid(gate) * up).astype(BF)

        lax.fori_loop(0, ff // step, columns, None)
        ready(2)
        out_ref[:] = (wide + nn(act_s[:], wd_s[:].reshape(ff, d)).astype(BF).astype(F32)).astype(BF)

    row = pl.BlockSpec((bt, d), lambda i: (i, 0))
    head = pl.BlockSpec((heads, bt, HEAD), lambda i: (0, i, 0))
    wider = lambda c: pl.BlockSpec((bt, c), lambda i: (i, 0))
    shape = lambda c, to: jax.ShapeDtypeStruct((t, c), to)
    scratch = [pltpu.VMEM((n, heads * HEAD // n, d), BF), pltpu.VMEM((n, d // n, 2 * ff), BF), pltpu.VMEM((n, ff // n, d), BF)]
    sems = [piece_sems(at)]
    inner = heads * HEAD
    if last:
        return pl.pallas_call(
            kernel, grid=(t // bt,), in_specs=[row, head, row, ANY], out_specs=[row, wider(ff), wider(2 * ff), row, head, ANY],
            out_shape=[shape(d, BF), shape(ff, BF), shape(2 * ff, BF), shape(d, BF), jax.ShapeDtypeStruct((heads, t, HEAD), BF),
                       jax.ShapeDtypeStruct((n, rows, WIDE), BF)],
            scratch_shapes=scratch + sum_scratch(inner, d, n) + sems, cost_estimate=cost(2 * t * d * (2 * d + 5 * ff), [h] * 20), compiler_params=params("arbitrary"),
        )(h, o, dy, source)
    return pl.pallas_call(
        kernel, grid=(t // bt,), in_specs=[row, head, ANY], out_specs=[row, wider(ff), wider(ff), row],
        out_shape=[shape(d, BF), shape(ff, F32), shape(ff, F32), shape(d, BF)],
        scratch_shapes=scratch + [pltpu.VMEM((bt, ff), BF)] + sems, cost_estimate=cost(2 * t * d * (d + 3 * ff), [h] * 20),
        compiler_params=params("arbitrary"))(h, o, source)


def back(dy, b, wide, scale, gate_ref, up_ref, wgu_s, wd_s, wo_s, act_ref, dgu_ref, dh2_ref, do_ref, heads, ff, step, mixed=None, acc_s=None,
         ready=None):
    d = dy.shape[1]
    n = wd_s.shape[0]
    own = ff // n
    by_b = None
    for c in range(0, ff, step):
        gate = nn(b, wgu_s[:, :, c : c + step].reshape(d, step)) if gate_ref is None else gate_ref[:, c : c + step]
        up = nn(b, wgu_s[:, :, ff + c : ff + c + step].reshape(d, step)) if up_ref is None else up_ref[:, c : c + step]
        by_act = nt(dy, wd_s[c // own : (c + step) // own].reshape(step, d)).astype(BF).astype(F32)
        if ready is not None and c == 0:
            ready(1)
        s = jax.nn.sigmoid(gate)
        silu = gate * s
        act_ref[:, c : c + step] = (silu * up).astype(BF)
        by_up = (by_act * silu).astype(BF)
        by_gate = (by_act * up * (s + silu * (1 - s))).astype(BF)
        dgu_ref[:, c : c + step] = by_gate
        dgu_ref[:, ff + c : ff + c + step] = by_up
        term = nt(by_gate, wgu_s[:, :, c : c + step].reshape(d, step)) + nt(by_up, wgu_s[:, :, ff + c : ff + c + step].reshape(d, step))
        by_b = term if by_b is None else by_b + term
    by_h2 = (dy.astype(F32) + norm_back(wide, scale, by_b)).astype(BF)
    dh2_ref[:] = by_h2
    if mixed is not None:
        add_grad(acc_s, mixed, by_h2)
    if ready is not None:
        ready(2)
    by_o = nt(by_h2, wo_s[:].reshape(-1, d)).astype(BF)
    for i in range(heads):
        do_ref[i] = by_o[:, i * HEAD : (i + 1) * HEAD]


def feed_back(dy, h2, gate, up, source, first, at, heads, tile=512):
    t, d = h2.shape
    n = source.shape[0]
    ff = gate.shape[1]
    bt, step = _fit(t, tile), _fit(ff, 512)

    def kernel(dy_ref, h2_ref, gate_ref, up_ref, w_ref, b_ref, act_ref, dgu_ref, dh2_ref, do_ref, wo_s, wgu_s, wd_s, sem):
        start = pl.program_id(0) == 0
        groups = [pieces_of(w_ref, first, at, "w_down", wd_s, 0, sem),
                  pieces_of(w_ref, first, at, "w_gate", wgu_s, 0, sem) + pieces_of(w_ref, first, at, "w_up", wgu_s, ff, sem),
                  pieces_of(w_ref, first, at, "wo", wo_s, 0, sem)]

        def ready(i):
            @pl.when(start)
            def _():
                for copy in groups[i]:
                    copy.wait()

        @pl.when(start)
        def _():
            for group in groups:
                for copy in group:
                    copy.start()

        ready(0)
        wide = h2_ref[:].astype(F32)
        scale = scale_of(wide)
        b_ref[:] = (wide * scale).astype(BF)
        back(dy_ref[:], None, wide, scale, gate_ref, up_ref, wgu_s, wd_s, wo_s, act_ref, dgu_ref, dh2_ref, do_ref, heads, ff, step,
             ready=ready)

    row = pl.BlockSpec((bt, d), lambda i: (i, 0))
    head = pl.BlockSpec((heads, bt, HEAD), lambda i: (0, i, 0))
    wider = lambda c: pl.BlockSpec((bt, c), lambda i: (i, 0))
    shape = lambda c: jax.ShapeDtypeStruct((t, c), BF)
    return pl.pallas_call(
        kernel, grid=(t // bt,), in_specs=[row, row, wider(ff), wider(ff), ANY], out_specs=[row, wider(ff), wider(2 * ff), row, head],
        out_shape=[shape(d), shape(ff), shape(2 * ff), shape(d), jax.ShapeDtypeStruct((heads, t, HEAD), BF)],
        scratch_shapes=[pltpu.VMEM((n, heads * HEAD // n, d), BF), pltpu.VMEM((n, d // n, 2 * ff), BF), pltpu.VMEM((n, ff // n, d), BF)]
        + [piece_sems(at)],
        cost_estimate=cost(2 * t * d * (d + 3 * ff), [gate, up, h2, h2, h2, h2]), compiler_params=params("arbitrary"))(dy, h2, gate, up, source)


def turned_back(dq, dk, dv, cos, sin, a, n, rows, start, h=None, dh2=None, source=None, first=0, at=None):
    heads, t, _ = dq.shape
    kv, d = dk.shape[0], a.shape[1]
    bt = _fit(t, 512)
    wide = (heads + 2 * kv) * HEAD
    more = h is not None

    def kernel(*refs):
        dq_ref, dk_ref, dv_ref, c_ref, s_ref, a_ref = refs[:6]
        if more:
            h_ref, dh2_ref, w_ref, t_ref, dh_ref, acc_s, held_s, out_sem, x_s, w_s, sem = refs[6:]
            start_now = pl.program_id(0) == 0
            copies, column = [], 0
            for name in ORDER[4:]:
                copies += pieces_of(w_ref, first, at, name, w_s, column, sem)
                column += at[name][2] * WIDE

            @pl.when(start_now)
            def _():
                for copy in copies:
                    copy.start()
        else:
            t_ref, acc_s, held_s, out_sem, x_s = refs[6:]
        cos_, sin_ = c_ref[:], s_ref[:]
        for i in range(heads + kv):
            y = (dq_ref[i] if i < heads else dk_ref[i - heads]).astype(F32)
            x_s[:, i * HEAD : (i + 1) * HEAD] = (y * cos_ - pltpu.roll(y, HEAD // 2, 1) * sin_).astype(BF)
        for i in range(kv):
            x_s[:, (heads + kv + i) * HEAD : (heads + kv + i + 1) * HEAD] = dv_ref[i]
        add_grad(acc_s, a_ref[:], x_s[:])
        if more:
            @pl.when(start_now)
            def _():
                for copy in copies:
                    copy.wait()

            x = h_ref[:].astype(F32)
            by_a = nt(x_s[:], w_s[:].reshape(-1, wide))
            dh_ref[:] = (dh2_ref[:].astype(F32) + norm_back(x, scale_of(x), by_a)).astype(BF)

        @pl.when(pl.program_id(0) == pl.num_programs(0) - 1)
        def _():
            put_packed(acc_s, held_s, t_ref, start, n, out_sem)

    tab = pl.BlockSpec((bt, HEAD), lambda i: (i, 0))
    head = lambda c: pl.BlockSpec((c, bt, HEAD), lambda i: (0, i, 0))
    wider = lambda c: pl.BlockSpec((bt, c), lambda i: (i, 0))
    specs, given = [head(heads), head(kv), head(kv), tab, tab, wider(d)], [dq, dk, dv, cos, sin, a]
    outs, out_specs, scratch = [jax.ShapeDtypeStruct((n, rows, WIDE), BF)], [ANY], sum_scratch(d, wide, n) + [pltpu.VMEM((bt, wide), BF)]
    if more:
        specs += [wider(d), wider(d), ANY]
        given += [h, dh2, source]
        outs += [jax.ShapeDtypeStruct((t, d), BF)]
        out_specs += [wider(d)]
        scratch += [pltpu.VMEM((n, d // n, wide), BF), piece_sems(at)]
    return pl.pallas_call(kernel, grid=(t // bt,), in_specs=specs, out_specs=out_specs, out_shape=outs, scratch_shapes=scratch,
                          cost_estimate=cost(2 * t * d * wide * (1 + more), given), compiler_params=params("arbitrary"))(*given)


def gate_up_grad(b, dgu, n, rows, base, first):
    t, d = b.shape
    r = d // n
    two = 2
    width = two * WIDE

    def kernel(b_ref, x_ref, _, out_ref, t_s):
        @pl.when(pl.program_id(0) == 0)
        def _():
            t_s[:] = b_ref[:].T

        out = nn(t_s[:], x_ref[:]).astype(BF)
        for c in range(two):
            out_ref[:, c * r : (c + 1) * r, :] = out[:, c * WIDE : (c + 1) * WIDE].reshape(n, r, WIDE)

    return pl.pallas_call(
        kernel, grid=(dgu.shape[1] // width,), in_specs=[pl.BlockSpec((t, d), lambda i: (0, 0)), pl.BlockSpec((t, width), lambda i: (0, i)), ANY],
        out_specs=pl.BlockSpec((n, two * r, WIDE), lambda i: (0, first // (two * r) + i, 0)), out_shape=jax.ShapeDtypeStruct((n, rows, WIDE), BF),
        scratch_shapes=[pltpu.VMEM((d, t), BF)], input_output_aliases={2: 0},
        cost_estimate=cost(2 * t * d * dgu.shape[1], [b, dgu]), compiler_params=params("arbitrary"))(b, dgu, base)


def down_grad(act, dy, n, rows, base, first):
    t, ff = act.shape
    d = dy.shape[1]
    r, count = ff // n, d // WIDE
    owners = 4

    def kernel(act_ref, dy_ref, _, out_ref):
        out = nn(act_ref[:].T, dy_ref[:]).astype(BF)
        for c in range(count):
            out_ref[:, c * r : (c + 1) * r, :] = out[:, c * WIDE : (c + 1) * WIDE].reshape(owners, r, WIDE)

    return pl.pallas_call(
        kernel, grid=(n // owners,), in_specs=[pl.BlockSpec((t, owners * r), lambda i: (0, i)), pl.BlockSpec((t, d), lambda i: (0, 0)), ANY],
        out_specs=pl.BlockSpec((owners, count * r, WIDE), lambda i: (i, first // (count * r), 0)), out_shape=jax.ShapeDtypeStruct((n, rows, WIDE), BF),
        input_output_aliases={2: 0}, cost_estimate=cost(2 * t * d * ff, [act, dy]), compiler_params=params("arbitrary"))(act, dy, base)


def mixed_grad(o, dh2, n, base, first):
    heads, t, _ = o.shape
    inner, columns = heads * HEAD, dh2.shape[1]

    def kernel(o_ref, x_ref, _, out_ref, t_s):
        @pl.when(pl.program_id(0) == 0)
        def _():
            for k in range(heads):
                t_s[k * HEAD : (k + 1) * HEAD, :] = o_ref[k].T

        out_ref[:] = nn(t_s[:], x_ref[:]).astype(BF).reshape(n, inner // n, WIDE)

    return pl.pallas_call(
        kernel, grid=(columns // WIDE,), in_specs=[pl.BlockSpec(o.shape, lambda i: (0, 0, 0)), pl.BlockSpec((t, WIDE), lambda i: (0, i)), ANY],
        out_specs=pl.BlockSpec((n, inner // n, WIDE), lambda i: (0, first // (inner // n) + i, 0)), out_shape=jax.ShapeDtypeStruct(base.shape, BF),
        scratch_shapes=[pltpu.VMEM((inner, t), BF)], input_output_aliases={2: 0},
        cost_estimate=cost(2 * t * inner * columns, [o, dh2]), compiler_params=params("arbitrary"))(o, dh2, base)


def adamw(total, count, weights, m, v, gradients, where):
    layers = weights["wq"].shape[0]
    units = [(name, number) for number in range(layers) for name in ORDER]

    def kernel(total_ref, *refs):
        k = len(gradients)
        g_refs, ins, outs = refs[:k], refs[k : k + 21], refs[k + 21 : k + 42]
        held, (in_sem, out_sem) = refs[k + 42 : k + 63], refs[k + 63 :]

        def moves(u, back):
            name, number = units[u]
            i = ORDER.index(name)
            for part in range(3):
                far, near = (outs if back else ins)[part * 7 + i].at[number], held[part * 7 + i].at[number]
                yield pltpu.make_async_copy(near, far, out_sem.at[u, part]) if back else pltpu.make_async_copy(far, near, in_sem.at[u, part])

        for u in range(len(units)):
            for copy in moves(u, False):
                copy.start()
        mean = jnp.sum(jnp.sum(total_ref[:], axis=0, keepdims=True), axis=1, keepdims=True) * (1.0 / count)
        factor = jnp.minimum(1.0, 0.5 * lax.rsqrt(mean + 1e-30))
        for u, (name, number) in enumerate(units):
            for copy in moves(u, False):
                copy.wait()
            which, first = where[name, number]
            w_s, m_s, v_s = (held[part * 7 + ORDER.index(name)] for part in range(3))
            _, r, c = weights[name].shape
            for j in range(c // WIDE):
                cut = (number, slice(None), slice(j * WIDE, (j + 1) * WIDE))
                g = g_refs[which][first + j * r : first + (j + 1) * r, :].astype(F32) * factor
                m_new = 0.9 * m_s[cut] + 0.1 * g
                v_new = 0.95 * v_s[cut] + 0.05 * g * g
                w = w_s[cut].astype(F32)
                w_s[cut] = (w - 0.02 * (m_new * lax.rsqrt(v_new + 1e-8) + 0.1 * w)).astype(BF)
                m_s[cut] = m_new
                v_s[cut] = v_new
            for copy in moves(u, True):
                copy.start()
        for u in range(len(units)):
            for copy in moves(u, True):
                copy.wait()

    given = [group[name] for group in (weights, m, v) for name in ORDER]
    out = pl.pallas_call(
        kernel, in_specs=[WHOLE] * (1 + len(gradients)) + [ANY] * 21, out_specs=[ANY] * 21,
        out_shape=[jax.ShapeDtypeStruct(x.shape, x.dtype) for x in given],
        scratch_shapes=[pltpu.VMEM(x.shape, x.dtype) for x in given] + [pltpu.SemaphoreType.DMA((len(units), 3))] * 2,
        compiler_params=params())(total, *gradients, *given)
    return [dict(zip(ORDER, out[i : i + 7])) for i in (0, 7, 14)]


def solution(mesh):
    n = mesh.shape["dp"]
    side = math.isqrt(n)

    def step(x, dy, *arrays):
        weights, m, v = (dict(zip(NAMES, arrays[i : i + 7], strict=True)) for i in (0, 7, 14))
        layers = weights["wq"].shape[0]
        at, rows = layout(weights)
        middle, late = at["wo"][0], at["wq"][0]
        heads, kv = weights["wq"].shape[2] // HEAD, weights["wk"].shape[2] // HEAD
        cos, sin = (jnp.asarray(one) for one in table(x.shape[1]))
        blocks, late_blocks = packed(weights, at, rows, late)
        whole = [lax.all_gather(block, "dp", axis=0, tiled=False) for block in blocks]
        first = gathered_now(side, late_blocks[0], 0)
        h, kept, by_h = x[0], [], dy[0]
        for number in range(layers):
            a, q, k, val = project(h, cos, sin, first, late, at, heads, kv)
            o, lse = attend(q, k, val)
            keep = dict(h=h, a=a, q=q, k=k, v=val, o=o, lse=lse, first=first)
            if number < layers - 1:
                block, _ = lax.optimization_barrier((late_blocks[number + 1], lse))
                o, first = lax.optimization_barrier((o, gathered_now(side, block, number + 1)))
                keep["h2"], keep["gate"], keep["up"], h = feed(h, o, whole[number], 0, at)
            else:
                result = feed(h, o, whole[number], 0, at, dy=by_h, rows=late)
            kept.append(keep)
        gradients, where = [], {}
        for number in reversed(range(layers)):
            keep, final = kept[number], number == layers - 1
            if final:
                b, act, dgu, dh2, do, terms = result
            else:
                b, act, dgu, dh2, do = feed_back(by_h, keep["h2"], keep["gate"], keep["up"], whole[number], 0, at, heads)
            total_rows = terms.shape[1]
            for name in ORDER[: 3 + final]:
                where[name, number] = (len(gradients), at[name][0])
            for name in ORDER[4 - (number < layers - 2) :] if not final else ():
                where[name, number + 1] = (len(gradients), at[name][0] - shift)
            terms = gate_up_grad(b, dgu, n, total_rows, terms, 0)
            terms = down_grad(act, by_h, n, total_rows, terms, at["w_down"][0])
            gradients.append(lax.psum_scatter(terms.reshape(n * total_rows, WIDE), "dp", scatter_dimension=0, tiled=True))
            dq, dk, dv = attend_bwd(keep["q"], keep["k"], keep["v"], do, keep["lse"], keep["o"])
            shift = late - middle if final else 0
            begin = (middle if number else 0) + late - middle - shift
            more = (keep["h"], dh2, keep["first"], late, at) if number else ()
            terms, *by_x = turned_back(dq, dk, dv, cos, sin, keep["a"], n, (middle if number else 0) + rows - middle - shift, begin, *more)
            if number:
                by_h = by_x[0]
            if not final:
                terms = mixed_grad(keep["o"], dh2, n, terms, begin - (late - middle))
        for name in ORDER[3:]:
            where[name, 0] = (len(gradients), at[name][0] - middle)
        g, part = summed_now(side, terms, gradients[:-1], layers)
        total = squares_now(n, part, gradients[-1], layers + 1)
        gradients.append(g)
        count = n * sum(w.size for w in weights.values())
        new = adamw(total, count, weights, m, v, gradients, where)
        return tuple(one[name] for one in new for name in NAMES)

    states, cut = P(("rep", "dp"), None, None), P(None, "dp", None)
    return jax.shard_map(
        step,
        mesh=mesh,
        in_specs=(states, states) + (cut,) * 21,
        out_specs=(P("rep", "dp", None),) * 21,
        check_vma=False,
    )
```
